32 devices in a mesh: fsdp: 2 (over x), ctx: 4 (over y, core), tp: 4 (over z).
Axes of the slice: x: 2, y: 2, z: 4, core: 2. Of those that a mesh axis runs over, the one named last changes fastest.
Arguments:
- hidden_in: bfloat16 [32, 512, 768], P('fsdp', 'ctx'), may hold values from -6 to 6
- lengths: int32 [32], P('fsdp'), may hold values from 128 to 512, as said below
- cotangent: bfloat16 [32, 512, 768], P('fsdp', 'ctx'), may hold values from -6 to 6
- w_qkv: bfloat16 [768, 3, 768], P(('fsdp', 'ctx'), None, 'tp'), may hold values from -0.21875 to 0.21875
- b_qv: bfloat16 [2, 768], P(None, 'tp'), may hold values from -1.5 to 1.5
- w_out: bfloat16 [768, 768], P('tp', ('fsdp', 'ctx')), may hold values from -2.5 to 2.5
- b_out: bfloat16 [768], P(('fsdp', 'ctx')), may hold values from -1.5 to 1.5
- gain_one: bfloat16 [768], P(('fsdp', 'ctx')), may hold values from 0.5 to 1.5
- shift_one: bfloat16 [768], P(('fsdp', 'ctx')), may hold values from -1.5 to 1.5
- w_in: bfloat16 [768, 3072], P(('fsdp', 'ctx'), 'tp'), may hold values from -0.21875 to 0.21875
- b_in: bfloat16 [3072], P('tp'), may hold values from -1.5 to 1.5
- w_down: bfloat16 [3072, 768], P('tp', ('fsdp', 'ctx')), may hold values from -0.109375 to 0.109375
- b_down: bfloat16 [768], P(('fsdp', 'ctx')), may hold values from -1.5 to 1.5
- gain_two: bfloat16 [768], P(('fsdp', 'ctx')), may hold values from 0.5 to 1.5
- shift_two: bfloat16 [768], P(('fsdp', 'ctx')), may hold values from -1.5 to 1.5
Outputs:
- hidden_out: bfloat16 [32, 512, 768], P('fsdp', 'ctx')
- grad_in: bfloat16 [32, 512, 768], P('fsdp', 'ctx')
- grad_w_qkv: float32 [768, 3, 768], P(('fsdp', 'ctx'), None, 'tp')
- grad_b_qv: float32 [2, 768], P(None, 'tp')
- grad_w_out: float32 [768, 768], P('tp', ('fsdp', 'ctx'))
- grad_b_out: float32 [768], P(('fsdp', 'ctx'))
- grad_gain_one: float32 [768], P(('fsdp', 'ctx'))
- grad_shift_one: float32 [768], P(('fsdp', 'ctx'))
- grad_w_in: float32 [768, 3072], P(('fsdp', 'ctx'), 'tp')
- grad_b_in: float32 [3072], P('tp')
- grad_w_down: float32 [3072, 768], P('tp', ('fsdp', 'ctx'))
- grad_b_down: float32 [768], P(('fsdp', 'ctx'))
- grad_gain_two: float32 [768], P(('fsdp', 'ctx'))
- grad_shift_two: float32 [768], P(('fsdp', 'ctx'))
The draws below stay inside these ranges and needn't reach their ends.
Inputs may be any that keep to these rules, and one draw needn't show every extreme that they name: The first lengths[s] positions of slot s are valid, the rest padding; some slot has 512 and some 512 // 4.
All inputs are finite; a program needn't handle non-finite values.
Results may differ from the reference program's by a relative error of at most 0.015.
The reference program's roundings to bfloat16 on the way count: a program that leaves them out, or rounds other values in their place, can miss the bound.
Values may be sent and summed in bfloat16 or wider, within the bound.
A program may use at most 192 MiB of HBM per device.

```python
import jax
import jax.numpy as jnp
from jax import lax

D = 768
HEADS = 12
HD = 64
FF = 3072
SEQ = 512
SLOTS = 32


def draw_lengths(key, part):
    key_base, key_top, key_gap = jax.random.split(key, 3)
    drawn = jax.random.randint(key_base, (SLOTS,), SEQ // 4, SEQ + 1)
    longest = jax.random.randint(key_top, (), 0, SLOTS)
    offset = jax.random.randint(key_gap, (), 1, SLOTS)
    shortest = (longest + offset) % SLOTS
    places = jnp.arange(SLOTS, dtype=jnp.int32)
    drawn = jnp.where(places == longest, SEQ, drawn)
    drawn = jnp.where(places == shortest, SEQ // 4, drawn)
    return drawn.astype(jnp.int32)


def raised(values, key, source, target, blocks, factor):
    owner, partner = [(jnp.arange(values.shape[position]) // (values.shape[position] // blocks)).reshape([-1 if axis == position else 1 for axis in range(values.ndim)]) for position in (source, target)]
    chosen = jax.random.permutation(key, blocks)[partner]
    strong = (owner == chosen) | (owner == (partner + blocks // 2) % blocks)
    return jnp.where(strong, factor * values, values)


def steps_of(stream_key, extent, pieces, smallest, top_value):
    loudness = 1.0
    for dim, parts in pieces:
        steps = jax.random.uniform(jax.random.fold_in(jax.random.fold_in(stream_key, 6), dim), (parts,), jnp.float32, smallest / len(pieces), top_value / len(pieces))
        loudness = loudness * jnp.repeat(jnp.exp(steps), extent[dim] // parts).reshape((-1,) + (1,) * (len(extent) - 1 - dim))
    return loudness


def bell_draw(stream_key, dims, spread, reach, shards=(), kind=jnp.bfloat16):
    gain = steps_of(stream_key, dims, shards, -0.22, 0.18) if shards else 1.0
    result = jax.random.normal(stream_key, dims, jnp.float32) * spread * gain
    return jnp.minimum(jnp.maximum(result, -reach), reach).astype(kind)


def heavy_noise(own_key, shape, width, reach, pieces, heavy, kind=jnp.bfloat16):
    values = width * jax.random.normal(own_key, shape, jnp.float32)
    if pieces:
        values = values * steps_of(own_key, shape, pieces, -0.22, 0.18)
    return jnp.clip(raised(values, jax.random.fold_in(own_key, 3), *heavy), -reach, reach).astype(kind)


def setup_inputs(seed: int = 0) -> dict:
    key_list = jax.random.split(jax.random.key(seed), 16)
    hidden_in = heavy_noise(key_list[0], (SLOTS, SEQ, D), 1.0, 6.0, ((0, 2), (1, 4)), (1, 2, 4, 2.0))
    lengths = draw_lengths(jax.random.fold_in(key_list[15], 71), 0)
    cotangent = bell_draw(key_list[2], (SLOTS, SEQ, D), 1.0, 6.0, ((0, 2), (1, 4)))
    w_qkv = bell_draw(key_list[3], (D, 3, D), D ** -0.5, 0.21875, ((0, 8), (2, 4)))
    b_qv = bell_draw(key_list[4], (2, D), 0.3, 1.5, ((1, 4),))
    w_out = bell_draw(key_list[5], (D, D), (max(D * 4 // SEQ, 1)) ** -0.5, 2.5, ((0, 4), (1, 8)))
    b_out = bell_draw(key_list[6], (D,), 0.3, 1.5, ((0, 8),))
    gain_one = jnp.clip(1.0 + 0.1 * jax.random.normal(key_list[7], (D,), jnp.float32), 0.5, 1.5).astype(jnp.bfloat16)
    shift_one = bell_draw(key_list[8], (D,), 0.3, 1.5, ((0, 8),))
    w_in = bell_draw(key_list[9], (D, FF), D ** -0.5, 0.21875, ((0, 8), (1, 4)))
    b_in = bell_draw(key_list[10], (FF,), 0.3, 1.5, ((0, 4),))
    w_down = bell_draw(key_list[11], (FF, D), FF ** -0.5, 0.109375, ((0, 4), (1, 8)))
    b_down = bell_draw(key_list[12], (D,), 0.3, 1.5, ((0, 8),))
    gain_two = jnp.clip(1.0 + 0.1 * jax.random.normal(key_list[13], (D,), jnp.float32), 0.5, 1.5).astype(jnp.bfloat16)
    shift_two = bell_draw(key_list[14], (D,), 0.3, 1.5, ((0, 8),))
    return {"hidden_in": hidden_in, "lengths": lengths, "cotangent": cotangent, "w_qkv": w_qkv, "b_qv": b_qv, "w_out": w_out, "b_out": b_out, "gain_one": gain_one, "shift_one": shift_one, "w_in": w_in, "b_in": b_in, "w_down": w_down, "b_down": b_down, "gain_two": gain_two, "shift_two": shift_two}


@jax.custom_vjp
def low(v):
    return lax.optimization_barrier(v.astype(jnp.bfloat16)).astype(jnp.float32)

@jax.custom_vjp
def low_back(v):
    return v

def low_keep(v):
    return (low(v), None)

def low_pass(kept, grad):
    return (grad,)

def back_keep(v):
    return (v, None)

def back_low(kept, grad):
    return (low(grad),)
low.defvjp(low_keep, low_pass)
low_back.defvjp(back_keep, back_low)
precise = lax.Precision.HIGHEST
epsilon = 1e-05

def layer_norm(summed, gain_row, shift_row):
    center = summed - lax.optimization_barrier(jnp.mean(summed, axis=-1, keepdims=True))
    variance = lax.optimization_barrier(jnp.mean(center * center, axis=-1, keepdims=True))
    return center * lax.rsqrt(variance + epsilon) * gain_row + shift_row

def one_slot(weights_now, tokens, length):
    w_qkv, b_qv, w_out, b_out, gain_one, shift_one, w_in, b_in, w_down, b_down, gain_two, shift_two = weights_now
    key_count = tokens.shape[0]
    bias_three = jnp.stack([b_qv[0], jnp.zeros_like(b_qv[0]), b_qv[1]])
    mixed = jnp.einsum('sd,dcf->scf', low(tokens), w_qkv, precision=precise) + bias_three
    mixed = low(low_back(mixed))
    queries = mixed[:, 0].reshape(key_count, HEADS, HD)
    keys_all = mixed[:, 1].reshape(key_count, HEADS, HD)
    values_all = mixed[:, 2].reshape(key_count, HEADS, HD)
    scores = low_back(jnp.einsum('qhe,khe->hqk', queries, keys_all, precision=precise) * HD ** (-0.5))
    key_valid = jnp.arange(key_count, dtype=jnp.int32) < length
    scores = jnp.where(key_valid[None, None, :], scores, -1e+30)
    probs = jax.nn.softmax(scores, axis=-1)
    context = jnp.einsum('hqk,khe->qhe', low(probs), values_all, precision=precise).reshape(key_count, HEADS * HD)
    context = low(low_back(context))
    attended = low_back(jnp.dot(context, w_out, precision=precise) + b_out)
    first_out = layer_norm(tokens + attended, gain_one, shift_one)
    pre_act = low_back(jnp.dot(low(first_out), w_in, precision=precise) + b_in)
    activated = low(jax.nn.gelu(pre_act, approximate=False))
    branch = low_back(jnp.dot(activated, w_down, precision=precise) + b_down)
    return layer_norm(first_out + branch, gain_two, shift_two)

def reference(hidden_in, lengths, cotangent, w_qkv, b_qv, w_out, b_out, gain_one, shift_one, w_in, b_in, w_down, b_down, gain_two, shift_two):
    weights_all = tuple((member.astype(jnp.float32) for member in (w_qkv, b_qv, w_out, b_out, gain_one, shift_one, w_in, b_in, w_down, b_down, gain_two, shift_two)))
    tokens_all = hidden_in.astype(jnp.float32)
    row_valid = (jnp.arange(SEQ, dtype=jnp.int32)[None, :] < lengths[:, None]).astype(jnp.float32)
    incoming = cotangent.astype(jnp.float32) * row_valid[:, :, None]

    def forward(weights_now, tokens_now):

        def slot_step(carried, packed):
            return (carried, one_slot(weights_now, packed[0], packed[1]))
        _, results = lax.scan(jax.checkpoint(slot_step), jnp.zeros((), jnp.float32), (tokens_now, lengths))
        return results
    output, pullback = jax.vjp(forward, weights_all, tokens_all)
    grad_weights, grad_tokens = pullback(incoming)
    return (output.astype(jnp.bfloat16), grad_tokens.astype(jnp.bfloat16), grad_weights[0], grad_weights[1], grad_weights[2], grad_weights[3], grad_weights[4], grad_weights[5], grad_weights[6], grad_weights[7], grad_weights[8], grad_weights[9], grad_weights[10], grad_weights[11])
```

```python
import jax
import jax.numpy as jnp
from jax import lax
from jax.experimental import pallas as pl
from jax.experimental.pallas import tpu as pltpu
from jax.sharding import PartitionSpec as P

HD = 64
SLOT_MB = 4


epsilon = 1e-05


def tp_total(partial_sum):
    return lax.psum(partial_sum, "tp")


def layer_norm(summed, gain_row, shift_row):
    center = summed - jnp.mean(summed, axis=-1, keepdims=True)
    inverse = lax.rsqrt(jnp.mean(center * center, axis=-1, keepdims=True) + epsilon)
    normed = center * inverse
    return (normed * gain_row + shift_row, normed, inverse)


def norm_back(incoming, normed, inverse, gain_row):
    scaled = incoming * gain_row
    result = inverse * (
        scaled
        - jnp.mean(scaled, axis=-1, keepdims=True)
        - normed * jnp.mean(scaled * normed, axis=-1, keepdims=True)
    )
    return (result, jnp.sum(incoming * normed, axis=0), jnp.sum(incoming, axis=0))


def attn_scores(queries, keys_all, key_valid, score_scale):
    raw_scores = (
        jnp.einsum("bqhe,bkhe->bhqk", queries, keys_all, preferred_element_type=jnp.float32)
        * score_scale
    )
    return jnp.where(key_valid[:, None, None, :], raw_scores, -1e30)


def on_device(
    hidden_in,
    lengths,
    cotangent,
    w_qkv,
    b_qv,
    w_out,
    b_out,
    gain_one,
    shift_one,
    w_in,
    b_in,
    w_down,
    b_down,
    gain_two,
    shift_two,
):
    local_slots, row_count, model_width = hidden_in.shape
    slot_batch = SLOT_MB
    micro_count = local_slots // slot_batch
    flat_rows = slot_batch * row_count
    key_count = row_count * lax.axis_size("ctx")
    local_width = w_qkv.shape[2]
    head_count = local_width // HD
    score_scale = HD ** (-0.5)
    row_place = lax.axis_index("ctx") * row_count + jnp.arange(row_count, dtype=jnp.int32)
    key_place = jnp.arange(key_count, dtype=jnp.int32)
    bias_three = jnp.stack([b_qv[0], jnp.zeros_like(b_qv[0]), b_qv[1]]).astype(jnp.float32)
    bias_in = b_in.astype(jnp.float32)
    bias_grads = (jnp.zeros((2, local_width), jnp.float32), jnp.zeros(b_in.shape, jnp.float32))
    outputs = []
    input_grads = []
    for micro_index in range(micro_count):
        gathered = (
            lax.all_gather(w_qkv, ("fsdp", "ctx"), axis=0, tiled=True),
            lax.all_gather(w_out, ("fsdp", "ctx"), axis=1, tiled=True),
            lax.all_gather(w_in, ("fsdp", "ctx"), axis=0, tiled=True),
            lax.all_gather(w_down, ("fsdp", "ctx"), axis=1, tiled=True),
            lax.all_gather(b_out, ("fsdp", "ctx"), axis=0, tiled=True),
            lax.all_gather(gain_one, ("fsdp", "ctx"), axis=0, tiled=True),
            lax.all_gather(shift_one, ("fsdp", "ctx"), axis=0, tiled=True),
            lax.all_gather(b_down, ("fsdp", "ctx"), axis=0, tiled=True),
            lax.all_gather(gain_two, ("fsdp", "ctx"), axis=0, tiled=True),
            lax.all_gather(shift_two, ("fsdp", "ctx"), axis=0, tiled=True),
        )
        full_qkv, full_out, full_in, full_down = (
            gathered[0],
            gathered[1],
            gathered[2],
            gathered[3],
        )
        full_bout = gathered[4].astype(jnp.float32)
        full_gain_one = gathered[5].astype(jnp.float32)
        full_shift_one = gathered[6].astype(jnp.float32)
        full_bdown = gathered[7].astype(jnp.float32)
        full_gain_two = gathered[8].astype(jnp.float32)
        full_shift_two = gathered[9].astype(jnp.float32)
        first_slot = micro_index * slot_batch
        tokens = hidden_in[first_slot : first_slot + slot_batch].reshape(flat_rows, model_width)
        length = lengths[first_slot : first_slot + slot_batch]
        row_valid = (row_place[None, :] < length[:, None]).astype(jnp.float32).reshape(flat_rows)
        key_valid = key_place[None, :] < length[:, None]
        qkv_local = (
            jnp.einsum("sd,dcf->scf", tokens, full_qkv, preferred_element_type=jnp.float32)
            + bias_three
        ).astype(jnp.bfloat16)
        kv_local = qkv_local[:, 1:].reshape(slot_batch, row_count, 2, local_width)
        key_value = lax.all_gather(kv_local, "ctx", axis=1, tiled=True)
        queries = qkv_local[:, 0].reshape(slot_batch, row_count, head_count, HD)
        keys_all = key_value[:, :, 0].reshape(slot_batch, key_count, head_count, HD)
        values_all = key_value[:, :, 1].reshape(slot_batch, key_count, head_count, HD)
        scores = attn_scores(queries, keys_all, key_valid, score_scale)
        highest = jnp.max(scores, axis=-1, keepdims=True)
        exponent = jnp.exp(scores - highest)
        denominator = jnp.sum(exponent, axis=-1, keepdims=True)
        log_total = highest + jnp.log(denominator)
        probs_low = (exponent / denominator).astype(jnp.bfloat16)
        context = (
            jnp.einsum("bhqk,bkhe->bqhe", probs_low, values_all, preferred_element_type=jnp.float32)
            .astype(jnp.bfloat16)
            .reshape(flat_rows, local_width)
        )
        attended = (
            tp_total(jnp.dot(context, full_out, preferred_element_type=jnp.float32)) + full_bout
        )
        first_out, normed_one, inverse_one = layer_norm(
            tokens.astype(jnp.float32) + attended, full_gain_one, full_shift_one
        )
        first_low = first_out.astype(jnp.bfloat16)
        pre_act = jnp.dot(first_low, full_in, preferred_element_type=jnp.float32) + bias_in
        activated = jax.nn.gelu(pre_act, approximate=False).astype(jnp.bfloat16)
        branch = (
            tp_total(jnp.dot(activated, full_down, preferred_element_type=jnp.float32)) + full_bdown
        )
        result, normed_two, inverse_two = layer_norm(
            first_out + branch, full_gain_two, full_shift_two
        )
        outputs.append(result.astype(jnp.bfloat16).reshape(slot_batch, row_count, model_width))
        incoming = (
            cotangent[first_slot : first_slot + slot_batch]
            .reshape(flat_rows, model_width)
            .astype(jnp.float32)
            * row_valid[:, None]
        )
        grad_two, grad_gain_two, grad_shift_two = norm_back(
            incoming, normed_two, inverse_two, full_gain_two
        )
        grad_branch = grad_two.astype(jnp.bfloat16)
        grad_bdown = jnp.sum(grad_branch.astype(jnp.float32), axis=0)
        grad_wdown = jnp.einsum(
            "sf,sd->fd", activated, grad_branch, preferred_element_type=jnp.float32
        )
        grad_act = jnp.einsum(
            "sd,fd->sf", grad_branch, full_down, preferred_element_type=jnp.float32
        )
        _, gelu_back = jax.vjp(
            lambda inner_value: jax.nn.gelu(inner_value, approximate=False), pre_act
        )
        grad_pre = gelu_back(grad_act)[0].astype(jnp.bfloat16)
        grad_win = jnp.einsum("sd,sf->df", first_low, grad_pre, preferred_element_type=jnp.float32)
        grad_bin = jnp.sum(grad_pre.astype(jnp.float32), axis=0)
        grad_first = grad_two + tp_total(
            jnp.einsum("sf,df->sd", grad_pre, full_in, preferred_element_type=jnp.float32)
        )
        grad_one, grad_gain_one, grad_shift_one = norm_back(
            grad_first, normed_one, inverse_one, full_gain_one
        )
        grad_attended = grad_one.astype(jnp.bfloat16)
        grad_bout = jnp.sum(grad_attended.astype(jnp.float32), axis=0)
        grad_wout = jnp.einsum(
            "sf,sd->fd", context, grad_attended, preferred_element_type=jnp.float32
        )
        grad_context = (
            jnp.einsum("sd,fd->sf", grad_attended, full_out, preferred_element_type=jnp.float32)
            .astype(jnp.bfloat16)
            .reshape(slot_batch, row_count, head_count, HD)
        )
        scores_again = attn_scores(queries, keys_all, key_valid, score_scale)
        weights_back = jnp.exp(scores_again - log_total)
        grad_probs = jnp.einsum(
            "bqhe,bkhe->bhqk", grad_context, values_all, preferred_element_type=jnp.float32
        )
        grad_scores = (
            weights_back * (grad_probs - jnp.sum(grad_probs * weights_back, axis=-1, keepdims=True))
        ).astype(jnp.bfloat16)
        grad_query = (
            jnp.einsum("bhqk,bkhe->bqhe", grad_scores, keys_all, preferred_element_type=jnp.float32)
            * score_scale
        )
        grad_key = (
            jnp.einsum("bhqk,bqhe->bkhe", grad_scores, queries, preferred_element_type=jnp.float32)
            * score_scale
        )
        grad_value = jnp.einsum(
            "bhqk,bqhe->bkhe",
            weights_back.astype(jnp.bfloat16),
            grad_context,
            preferred_element_type=jnp.float32,
        )
        key_value_terms = jnp.stack(
            [
                grad_key.reshape(slot_batch, key_count, local_width),
                grad_value.reshape(slot_batch, key_count, local_width),
            ],
            axis=2,
        )
        key_value_grad = lax.psum_scatter(key_value_terms, "ctx", scatter_dimension=1, tiled=True)
        grad_qkv = (
            jnp.concatenate(
                [grad_query.reshape(slot_batch, row_count, 1, local_width), key_value_grad], axis=2
            )
            .astype(jnp.bfloat16)
            .reshape(flat_rows, 3, local_width)
        )
        grad_wqkv = jnp.einsum("sd,scf->dcf", tokens, grad_qkv, preferred_element_type=jnp.float32)
        qkv_sums = jnp.sum(grad_qkv.astype(jnp.float32), axis=0)
        grad_bqv = jnp.stack([qkv_sums[0], qkv_sums[2]])
        grad_tokens = grad_one + tp_total(
            jnp.einsum("scf,dcf->sd", grad_qkv, full_qkv, preferred_element_type=jnp.float32)
        )
        input_grads.append(
            grad_tokens.astype(jnp.bfloat16).reshape(slot_batch, row_count, model_width)
        )
        bias_grads = (bias_grads[0] + grad_bqv, bias_grads[1] + grad_bin)
        pieces = (
            lax.psum_scatter(grad_wqkv, ("fsdp", "ctx"), scatter_dimension=0, tiled=True),
            lax.psum_scatter(grad_wout, ("fsdp", "ctx"), scatter_dimension=1, tiled=True),
            lax.psum_scatter(grad_win, ("fsdp", "ctx"), scatter_dimension=0, tiled=True),
            lax.psum_scatter(grad_wdown, ("fsdp", "ctx"), scatter_dimension=1, tiled=True),
            lax.psum_scatter(grad_bout, ("fsdp", "ctx"), scatter_dimension=0, tiled=True),
            lax.psum_scatter(grad_gain_one, ("fsdp", "ctx"), scatter_dimension=0, tiled=True),
            lax.psum_scatter(grad_shift_one, ("fsdp", "ctx"), scatter_dimension=0, tiled=True),
            lax.psum_scatter(grad_bdown, ("fsdp", "ctx"), scatter_dimension=0, tiled=True),
            lax.psum_scatter(grad_gain_two, ("fsdp", "ctx"), scatter_dimension=0, tiled=True),
            lax.psum_scatter(grad_shift_two, ("fsdp", "ctx"), scatter_dimension=0, tiled=True),
        )
        grad_shards = pieces if micro_index == 0 else jax.tree.map(jnp.add, grad_shards, pieces)
    bias_total = lax.psum((bias_grads[0], bias_grads[1]), ("fsdp", "ctx"))
    return (
        jnp.concatenate(outputs, axis=0),
        jnp.concatenate(input_grads, axis=0),
        grad_shards[0],
        bias_total[0],
        grad_shards[1],
        grad_shards[4],
        grad_shards[5],
        grad_shards[6],
        grad_shards[2],
        bias_total[1],
        grad_shards[3],
        grad_shards[7],
        grad_shards[8],
        grad_shards[9],
    )


MESH = pl.DeviceIdType.MESH
ANY = pl.BlockSpec(memory_space=pl.ANY)
VM = pl.BlockSpec(memory_space=pltpu.VMEM)


class Place:
    def __init__(self):
        f, c, t = lax.axis_index("fsdp"), lax.axis_index("ctx"), lax.axis_index("tp")
        self.f, self.c, self.t = f, c, t
        core = c % 2
        self.core, self.y = core, c // 2
        self.c_core = c + 1 - 2 * core
        self.c_y = (c + 2) % 4
        self.x_dev = (1 - f, c, t)
        self.y_dev = (f, self.c_y, t)
        self.core_dev = (f, self.c_core, t)
        self.own = 4 * f + c
        self.own_core = 4 * f + self.c_core
        self.fc_x = 4 * (1 - f) + c
        self.fc_y = 4 * f + self.c_y
        self.fc_d = 4 * (1 - f) + self.c_y

    def z_dev(self, step):
        return (self.f, self.c, (self.t + step) % 4)

    def c_dev(self, step):
        return (self.f, (self.c + step) % 4, self.t)

    def barrier(self):
        sem = pltpu.get_barrier_semaphore()
        devs = [self.z_dev(s) for s in (1, 2, 3)] + [self.x_dev] + [self.c_dev(s) for s in (1, 2, 3)]
        for dev in devs:
            pl.semaphore_signal(sem, inc=1, device_id=dev, device_id_type=MESH)
        pl.semaphore_wait(sem, len(devs))


class Sends:
    def __init__(self, sems):
        self.sems, self.list = sems, []

    def start(self, src, dst, rsem, dev, cond=None):
        copy = pltpu.make_async_remote_copy(
            src_ref=src, dst_ref=dst, send_sem=self.sems.at[len(self.list)], recv_sem=rsem,
            device_id=dev, device_id_type=MESH)
        self.list.append((copy, cond))
        if cond is None:
            copy.start()
        else:
            pl.when(cond)(copy.start)

    def finish(self):
        for copy, cond in self.list:
            if cond is None:
                copy.wait_send()
            else:
                pl.when(cond)(copy.wait_send)


def arrived(ref, rsem, dev):
    pltpu.make_async_remote_copy(
        src_ref=ref, dst_ref=ref, send_sem=rsem, recv_sem=rsem, device_id=dev, device_id_type=MESH
    ).wait_recv()


def gather_kernel(hid, cot, *refs):
    nk = 4
    shard = refs[:nk]
    out = refs[nk:2 * nk]
    x_out, cot_out = refs[2 * nk:2 * nk + 2]
    ssem, rsem, xsem, lsem = refs[2 * nk + 2:]
    at = Place()
    at.barrier()
    sends = Sends(ssem)
    local = []
    for k in range(nk):
        local.append(pltpu.make_async_copy(shard[k], out[k].at[at.t, at.own], lsem.at[k]))
    for i, (src, dst) in enumerate(((hid, x_out), (cot, cot_out))):
        local.append(pltpu.make_async_copy(src.at[4 * at.t + at.c], dst.at[at.c], lsem.at[nk + i]))
    for copy in local:
        copy.start()

    def piece(k, t, fc):
        return out[k].at[t, fc], rsem.at[k, t, fc]

    def slots(i):
        src, dst = ((hid, x_out), (cot, cot_out))[i]
        for s in (2, 3, 1):
            sends.start(src.at[4 * at.t + (at.c + s) % 4], dst.at[at.c], xsem.at[i, at.c], at.c_dev(s))

    slots(0)
    for k in range(nk):
        for s in (1, 2, 3):
            dst, sem = piece(k, at.t, at.own)
            sends.start(shard[k], dst, sem, at.z_dev(s))
        if k == 1:
            for kk in (0, 1):
                dst, sem = piece(kk, at.t, at.own)
                for dev in (at.x_dev, at.y_dev, at.core_dev):
                    sends.start(shard[kk], dst, sem, dev)

    def forward(k, t, fc, devs):
        ref, sem = piece(k, t, fc)
        for dev in devs:
            sends.start(ref, ref, sem, dev)

    def z_in(k, s):
        tt = (at.t + s) % 4
        if s:
            arrived(*piece(k, tt, at.own), at.x_dev)
            forward(k, tt, at.own, (at.x_dev, at.y_dev, at.core_dev))
        elif k > 1:
            dst, sem = piece(k, at.t, at.own)
            for dev in (at.x_dev, at.y_dev, at.core_dev):
                sends.start(shard[k], dst, sem, dev)

    def xy_in(k, s):
        tt = (at.t + s) % 4
        arrived(*piece(k, tt, at.fc_x), at.x_dev)
        forward(k, tt, at.fc_x, (at.core_dev,) if s % 2 else (at.y_dev, at.core_dev))
        arrived(*piece(k, tt, at.fc_y), at.x_dev)
        forward(k, tt, at.fc_y, (at.x_dev, at.core_dev) if s % 2 else (at.core_dev,))

    def d_in(k, s):
        tt = (at.t + s) % 4
        arrived(*piece(k, tt, at.fc_d), at.x_dev)
        forward(k, tt, at.fc_d, (at.core_dev,))

    steps = [(k, s) for k in range(nk) for s in range(4)]
    n = len(steps)
    for i in range(n + 2):
        if i < n:
            z_in(*steps[i])
        if 1 <= i < n + 1:
            xy_in(*steps[i - 1])
        if 2 <= i < n + 2:
            d_in(*steps[i - 2])
        if i == n // 2:
            slots(1)
    for i in range(2):
        dst = (x_out, cot_out)[i]
        for s in (1, 2, 3):
            c = (at.c + s) % 4
            arrived(dst.at[c], xsem.at[i, c], at.x_dev)
    for k in range(nk):
        for s in range(4):
            for chip in range(4):
                arrived(*piece(k, (at.t + s) % 4, 2 * chip + 1 - at.core), at.x_dev)
    for copy in local:
        copy.wait()
    sends.finish()


def gather_all(hid, cot, shards):
    n_send = 4 * 31 + 6
    out_shape = [jax.ShapeDtypeStruct((4, 8) + s.shape, s.dtype) for s in shards]
    out_shape += [jax.ShapeDtypeStruct((4,) + hid.shape[1:], hid.dtype)] * 2
    return pl.pallas_call(
        gather_kernel,
        out_shape=out_shape,
        in_specs=[ANY, ANY] + [VM] * 4,
        out_specs=[ANY] * 6,
        scratch_shapes=[
            pltpu.SemaphoreType.DMA((n_send,)),
            pltpu.SemaphoreType.DMA((4, 4, 8)),
            pltpu.SemaphoreType.DMA((2, 4)),
            pltpu.SemaphoreType.DMA((6,)),
        ],
        compiler_params=pltpu.CompilerParams(collective_id=0, has_side_effects=True),
        name="gather_all",
    )(hid, cot, *shards)


def reduce_kernel(*refs):
    nk = 3
    grads = refs[:nk]
    vec, o_slots = refs[nk], refs[nk + 1:nk + 3]
    total = refs[nk + 3:2 * nk + 3]
    vec_out, outs = refs[2 * nk + 3], refs[2 * nk + 4:2 * nk + 6]
    rc, own, bx, by, dx, dy, bz, vbuf, ssem, csem, bsem, zsem, vsem, osem, lsem = refs[2 * nk + 6:]
    at = Place()
    at.barrier()
    sends = Sends(ssem)
    chips = (at.fc_d, at.fc_x, at.fc_y, at.own)
    local = []

    for i in range(2):
        copy = pltpu.make_async_copy(o_slots[i].at[at.c], outs[i].at[4 * at.t + at.c], lsem.at[i])
        copy.start()
        local.append(copy)

    def slot_out(i):
        slot = 4 * at.t + at.c
        for s in (2, 1, 3):
            sends.start(o_slots[i].at[(at.c + s) % 4], outs[i].at[slot], osem.at[i, slot], at.c_dev(s))

    def along(i, hop, src_c, src=None):
        slot_r = 4 * ((at.t - hop) % 4) + src_c
        slot_l = 4 * ((at.t + hop) % 4) + src_c
        if hop:
            @pl.when(at.t >= hop)
            def _():
                arrived(outs[i].at[slot_r], osem.at[i, slot_r], at.x_dev)

            @pl.when(at.t + hop <= 3)
            def _():
                arrived(outs[i].at[slot_l], osem.at[i, slot_l], at.x_dev)
        if hop < 3:
            ref = outs[i].at[slot_r] if src is None else src
            sends.start(ref, outs[i].at[slot_r], osem.at[i, slot_r], at.z_dev(1), (at.t >= hop) & (at.t < 3))
            ref = outs[i].at[slot_l] if src is None else src
            sends.start(ref, outs[i].at[slot_l], osem.at[i, slot_l], at.z_dev(3), (at.t + hop <= 3) & (at.t > 0))

    def along_own(i, s):
        c = (at.c + s) % 4
        if s == 0:
            along(i, 0, at.c, o_slots[i].at[at.c])
        else:
            slot = 4 * at.t + c
            arrived(outs[i].at[slot], osem.at[i, slot], at.x_dev)
            along(i, 0, c)

    def core_out(k):
        for r, fc in enumerate(chips):
            other = fc + 1 - 2 * at.core
            sends.start(grads[k].at[:, other], rc.at[k, r], csem.at[k, r], at.core_dev)

    def add_core(k, r):
        arrived(rc.at[k, r], csem.at[k, r], at.x_dev)
        fc = chips[r]

        @pl.loop(0, 4)
        def _(t):
            both = grads[k][t, fc].astype(jnp.float32) + rc[k, r, t].astype(jnp.float32)
            rc[k, r, t] = both.astype(jnp.bfloat16)

    def diag_out(k):
        add_core(k, 0)
        sends.start(rc.at[k, 0, pl.ds(0, 2)], dx.at[k], bsem.at[k, 0], at.x_dev)
        sends.start(rc.at[k, 0, pl.ds(2, 2)], dy.at[k], bsem.at[k, 1], at.y_dev)

    def side_out(k):
        add_core(k, 1)
        sends.start(rc.at[k, 1, pl.ds(0, 2)], bx.at[k, pl.ds(0, 2)], bsem.at[k, 2], at.x_dev)
        add_core(k, 2)
        sends.start(rc.at[k, 2, pl.ds(2, 2)], by.at[k, pl.ds(2, 2)], bsem.at[k, 3], at.y_dev)

    def relay(k):
        arrived(dy.at[k], bsem.at[k, 1], at.x_dev)

        @pl.loop(0, 2)
        def _(t):
            both = rc[k, 1, t + 2].astype(jnp.float32) + dy[k, t].astype(jnp.float32)
            rc[k, 1, t + 2] = both.astype(jnp.bfloat16)

        sends.start(rc.at[k, 1, pl.ds(2, 2)], bx.at[k, pl.ds(2, 2)], bsem.at[k, 4], at.x_dev)
        arrived(dx.at[k], bsem.at[k, 0], at.x_dev)

        @pl.loop(0, 2)
        def _(t):
            both = rc[k, 2, t].astype(jnp.float32) + dx[k, t].astype(jnp.float32)
            rc[k, 2, t] = both.astype(jnp.bfloat16)

        sends.start(rc.at[k, 2, pl.ds(0, 2)], by.at[k, pl.ds(0, 2)], bsem.at[k, 5], at.y_dev)

    def own_sum(k):
        add_core(k, 3)
        arrived(bx.at[k, pl.ds(0, 2)], bsem.at[k, 2], at.x_dev)
        arrived(by.at[k, pl.ds(2, 2)], bsem.at[k, 3], at.x_dev)
        arrived(bx.at[k, pl.ds(2, 2)], bsem.at[k, 4], at.x_dev)
        arrived(by.at[k, pl.ds(0, 2)], bsem.at[k, 5], at.x_dev)

        @pl.loop(0, 4)
        def _(t):
            four = rc[k, 3, t].astype(jnp.float32) + bx[k, t].astype(jnp.float32) + by[k, t].astype(jnp.float32)
            own[k, t] = four.astype(jnp.bfloat16)

        for s in (2, 1, 3):
            sends.start(own.at[k, (at.t + s) % 4], bz.at[k, s - 1], zsem.at[k, s - 1], at.z_dev(s))

    def last(k):
        for s in (1, 2, 3):
            arrived(bz.at[k, s - 1], zsem.at[k, s - 1], at.x_dev)

        @pl.loop(0, 6)
        def _(i):
            rows = pl.ds(pl.multiple_of(i * 16, 16), 16)
            value = own[k, at.t, rows].astype(jnp.float32)
            for s in range(3):
                value = value + bz[k, s, rows].astype(jnp.float32)
            total[k][rows] = value

    def vec_step(i):
        if i:
            arrived(vbuf.at[i - 1], vsem.at[i - 1], at.x_dev)
            vbuf[2 + i] = (vec[...] if i == 1 else vbuf[1 + i]) + vbuf[i - 1]
        if i < 3:
            sends.start(vec if i == 0 else vbuf.at[2 + i], vbuf.at[i], vsem.at[i], (at.core_dev, at.x_dev, at.y_dev)[i])
        else:
            for s in (1, 2, 3):
                sends.start(vbuf.at[5], vbuf.at[6 + at.t], vsem.at[3 + at.t], at.z_dev(s))

    def vec_last():
        for s in (1, 2, 3):
            t = (at.t + s) % 4
            arrived(vbuf.at[6 + t], vsem.at[3 + t], at.x_dev)
        vbuf[6 + at.t] = vbuf[5]
        vec_out[...] = vbuf[6] + vbuf[7] + vbuf[8] + vbuf[9]

    order = (2, 1, 0)
    slot_out(0)
    core_out(2)
    vec_step(0)
    along_own(0, 0)
    core_out(1)
    core_out(0)
    slot_out(1)
    for s in (1, 3, 2):
        along_own(0, s)
    diag_out(2)
    side_out(2)
    along_own(1, 0)
    for s in (1, 3, 2):
        along_own(1, s)
    jobs = [lambda: diag_out(1), lambda: side_out(1), lambda: relay(2), lambda: vec_step(1), lambda: diag_out(0),
            lambda: side_out(0), lambda: relay(1), lambda: vec_step(2), lambda: own_sum(2), lambda: relay(0),
            lambda: vec_step(3), lambda: own_sum(1), lambda: last(2), lambda: own_sum(0), lambda: last(1),
            lambda: vec_last(), lambda: last(0)]
    hops = [(i, hop, s) for hop in (1, 2, 3) for i in range(2) for s in range(4)]
    n = max(len(jobs), len(hops))
    for j in range(n):
        if j < len(jobs):
            jobs[j]()
        if j < len(hops):
            i, hop, s = hops[j]
            along(i, hop, (at.c + (0, 1, 3, 2)[s]) % 4)
    for copy in local:
        copy.wait()
    sends.finish()


def reduce_all(grads, vec, o_slots, slot_count):
    rows, width = grads[0].shape[2:]
    bf = jnp.bfloat16
    dma = pltpu.SemaphoreType.DMA
    n_send = 3 * (4 + 2 + 2 + 2 + 3) + 6 + 2 * (3 + 24)
    out_shape = [jax.ShapeDtypeStruct((rows, width), jnp.float32)] * 3
    out_shape += [jax.ShapeDtypeStruct(vec.shape, jnp.float32)]
    out_shape += [jax.ShapeDtypeStruct((slot_count,) + o_slots[0].shape[1:], bf)] * 2
    return pl.pallas_call(
        reduce_kernel,
        out_shape=out_shape,
        in_specs=[VM] * 6,
        out_specs=[VM] * 4 + [ANY] * 2,
        scratch_shapes=[
            pltpu.VMEM((3, 4, 4, rows, width), bf),
            pltpu.VMEM((3, 4, rows, width), bf),
            pltpu.VMEM((3, 4, rows, width), bf),
            pltpu.VMEM((3, 4, rows, width), bf),
            pltpu.VMEM((3, 2, rows, width), bf),
            pltpu.VMEM((3, 2, rows, width), bf),
            pltpu.VMEM((3, 3, rows, width), bf),
            pltpu.VMEM((10,) + vec.shape, jnp.float32),
            dma((n_send,)), dma((3, 4)), dma((3, 6)), dma((3, 3)), dma((7,)), dma((2, slot_count)), dma((2,)),
        ],
        compiler_params=pltpu.CompilerParams(collective_id=1, has_side_effects=True,
                                             vmem_limit_bytes=60 * 1024 * 1024),
        name="reduce_all",
    )(*grads, vec, *o_slots)


def one_slot(tokens, length, cotangent, mix, w_in, w_down_t, small):
    f32, bf16 = jnp.float32, jnp.bfloat16
    rows, model_width = tokens.shape
    groups, _, width = mix.shape
    part = width // 4
    per = part // HD
    score_scale = HD ** (-0.5)
    spot = jnp.arange(rows, dtype=jnp.int32)
    valid = spot < length
    small = small.astype(f32)
    bias_in, bias_qv = small[:, 0, 0], small[:, 0, 1]
    bout, gain_one, shift_one, bdown, gain_two, shift_two = [jnp.sum(small[0, :, 2 + i], axis=0) for i in range(6)]
    w_qkv = mix[:, :, : 3 * part]
    w_out_t = mix[:, :, 3 * part :]
    qkv = jnp.einsum("sd,tdn->tsn", tokens, w_qkv, preferred_element_type=f32) + bias_qv[:, None, : 3 * part]
    qkv = qkv.astype(bf16).reshape(groups, rows, 3, per, HD)
    queries, keys, values = qkv[:, :, 0], qkv[:, :, 1], qkv[:, :, 2]
    scores = jnp.einsum("tqhe,tkhe->thqk", queries, keys, preferred_element_type=f32) * score_scale
    scores = jnp.where(valid[None, None, None, :], scores, -1e30)
    highest = jnp.max(scores, axis=-1, keepdims=True)
    exponent = jnp.exp(scores - highest)
    denominator = jnp.sum(exponent, axis=-1, keepdims=True)
    probs = exponent / denominator
    probs_low = probs.astype(bf16)
    context = jnp.einsum("thqk,tkhe->tqhe", probs_low, values, preferred_element_type=f32).astype(bf16)
    context = context.reshape(groups, rows, part)
    attended = jnp.einsum("tsf,tdf->sd", context, w_out_t, preferred_element_type=f32) + bout
    first_out, normed_one, inverse_one = layer_norm(tokens.astype(f32) + attended, gain_one, shift_one)
    first_low = first_out.astype(bf16)
    pre_act = jnp.einsum("sd,tdf->tsf", first_low, w_in, preferred_element_type=f32) + bias_in[:, None, :]
    half = 0.5 * (1.0 + lax.erf(pre_act * (2.0 ** -0.5)))
    activated = (pre_act * half).astype(bf16)
    slope = half + pre_act * jnp.exp(-0.5 * pre_act * pre_act) * 0.3989422804014327
    branch = jnp.einsum("tsf,tdf->sd", activated, w_down_t, preferred_element_type=f32) + bdown
    result, normed_two, inverse_two = layer_norm(first_out + branch, gain_two, shift_two)
    incoming = cotangent.astype(f32) * valid.astype(f32)[:, None]
    grad_two, g_gain_two, g_shift_two = norm_back(incoming, normed_two, inverse_two, gain_two)
    grad_branch = grad_two.astype(bf16)
    g_bdown = jnp.sum(grad_branch.astype(f32), axis=0)
    g_down_t = jnp.einsum("sd,tsf->tdf", grad_branch, activated, preferred_element_type=f32).astype(bf16)
    grad_act = jnp.einsum("sd,tdf->tsf", grad_branch, w_down_t, preferred_element_type=f32)
    grad_pre = (grad_act * slope).astype(bf16)
    g_in = jnp.einsum("sd,tsf->tdf", first_low, grad_pre, preferred_element_type=f32).astype(bf16)
    g_bin = jnp.sum(grad_pre.astype(f32), axis=1)
    grad_first = grad_two + jnp.einsum("tsf,tdf->sd", grad_pre, w_in, preferred_element_type=f32)
    grad_one, g_gain_one, g_shift_one = norm_back(grad_first, normed_one, inverse_one, gain_one)
    grad_attended = grad_one.astype(bf16)
    g_bout = jnp.sum(grad_attended.astype(f32), axis=0)
    g_out_t = jnp.einsum("sd,tsf->tdf", grad_attended, context, preferred_element_type=f32).astype(bf16)
    grad_context = jnp.einsum("sd,tdf->tsf", grad_attended, w_out_t, preferred_element_type=f32).astype(bf16)
    grad_context = grad_context.reshape(groups, rows, per, HD)
    grad_probs = jnp.einsum("tqhe,tkhe->thqk", grad_context, values, preferred_element_type=f32)
    grad_scores = (probs * (grad_probs - jnp.sum(grad_probs * probs, axis=-1, keepdims=True))).astype(bf16)
    grad_query = jnp.einsum("thqk,tkhe->tqhe", grad_scores, keys, preferred_element_type=f32) * score_scale
    grad_key = jnp.einsum("thqk,tqhe->tkhe", grad_scores, queries, preferred_element_type=f32) * score_scale
    grad_value = jnp.einsum("thqk,tqhe->tkhe", probs_low, grad_context, preferred_element_type=f32)
    grad_qkv = jnp.concatenate(
        [part_grad.astype(bf16).reshape(groups, rows, part) for part_grad in (grad_query, grad_key, grad_value)],
        axis=2,
    )
    g_qkv = jnp.einsum("sd,tsn->tdn", tokens, grad_qkv, preferred_element_type=f32).astype(bf16)
    g_bqv = jnp.sum(grad_qkv.astype(f32), axis=1)
    grad_tokens = grad_one + jnp.einsum("tsn,tdn->sd", grad_qkv, w_qkv, preferred_element_type=f32)
    g_mix = jnp.concatenate([g_qkv, g_out_t], axis=2)
    vec = jnp.concatenate(
        [
            g_bin,
            jnp.pad(g_bqv, ((0, 0), (0, part))),
            jnp.stack([g_bout, g_gain_one, g_shift_one, g_bdown, g_gain_two, g_shift_two]),
            jnp.zeros((2, width), f32),
        ]
    )
    return result.astype(bf16), grad_tokens.astype(bf16), g_mix, g_in, g_down_t, vec


def slot_per_device(
    hidden_in, lengths, cotangent, w_qkv, b_qv, w_out, b_out, gain_one, shift_one, w_in, b_in, w_down, b_down,
    gain_two, shift_two,
):
    slot_count, block, model_width = hidden_in.shape
    rows, _, part = w_qkv.shape
    f, c, t = lax.axis_index("fsdp"), lax.axis_index("ctx"), lax.axis_index("tp")
    ctx = lax.axis_size("ctx")
    own = f * ctx + c
    mix = jnp.concatenate([w_qkv.reshape(rows, 3 * part), w_out.T], axis=1)
    vectors = jnp.stack([b_out, gain_one, shift_one, b_down, gain_two, shift_two])
    placed = jnp.where(
        jnp.arange(model_width, dtype=jnp.int32)[None, :] // rows == own, jnp.tile(vectors, (1, model_width // rows)), 0
    ).astype(jnp.bfloat16)
    gap = jnp.zeros((part,), jnp.bfloat16)
    small = jnp.concatenate(
        [
            b_in[None],
            jnp.concatenate([b_qv[0], gap, b_qv[1], gap])[None],
            placed,
            jnp.zeros((8, model_width), jnp.bfloat16),
        ]
    )
    small_all, mix_all, in_all, down_all, tokens, cot = gather_all(
        hidden_in, cotangent, (small, mix, w_in, w_down.T)
    )
    full = lambda g: g.reshape(g.shape[0], model_width, g.shape[3])
    length = lax.dynamic_index_in_dim(lengths, t * ctx + c, keepdims=False)
    result, grad_tokens, g_mix, g_in, g_down, vec = one_slot(
        tokens.reshape(ctx * block, model_width), length, cot.reshape(ctx * block, model_width),
        full(mix_all), full(in_all), full(down_all), small_all,
    )
    split = lambda g: g.reshape(g.shape[0], model_width // rows, rows, g.shape[2])
    back = lambda o: o.reshape(ctx, block, model_width)
    t_mix, t_in, t_down, t_vec, out, grad_in = reduce_all(
        (split(g_mix), split(g_in), split(g_down)), vec, (back(result), back(grad_tokens)), slot_count
    )
    piece = lax.dynamic_slice_in_dim(t_vec[8:14], own * rows, rows, axis=1)
    bqv = lax.dynamic_index_in_dim(t_vec, 4 + t, keepdims=False)
    bin_grad = lax.dynamic_index_in_dim(t_vec, t, keepdims=False)
    return (
        out,
        grad_in,
        t_mix[:, : 3 * part].reshape(rows, 3, part),
        jnp.stack([bqv[:part], bqv[2 * part : 3 * part]]),
        t_mix[:, 3 * part :].T,
        piece[0],
        piece[1],
        piece[2],
        t_in,
        bin_grad,
        t_down.T,
        piece[3],
        piece[4],
        piece[5],
    )


def solution(mesh):
    shape = mesh.shape
    whole_slots = (shape["fsdp"], shape["ctx"], shape["tp"]) == (2, 4, 4)
    return jax.shard_map(
        slot_per_device if whole_slots else on_device,
        mesh=mesh,
        in_specs=(
            P("fsdp", "ctx", None),
            P("fsdp"),
            P("fsdp", "ctx", None),
            P(("fsdp", "ctx"), None, "tp"),
            P(None, "tp"),
            P("tp", ("fsdp", "ctx")),
            P(("fsdp", "ctx")),
            P(("fsdp", "ctx")),
            P(("fsdp", "ctx")),
            P(("fsdp", "ctx"), "tp"),
            P("tp"),
            P("tp", ("fsdp", "ctx")),
            P(("fsdp", "ctx")),
            P(("fsdp", "ctx")),
            P(("fsdp", "ctx")),
        ),
        out_specs=(
            P("fsdp", "ctx", None),
            P("fsdp", "ctx", None),
            P(("fsdp", "ctx"), None, "tp"),
            P(None, "tp"),
            P("tp", ("fsdp", "ctx")),
            P(("fsdp", "ctx")),
            P(("fsdp", "ctx")),
            P(("fsdp", "ctx")),
            P(("fsdp", "ctx"), "tp"),
            P("tp"),
            P("tp", ("fsdp", "ctx")),
            P(("fsdp", "ctx")),
            P(("fsdp", "ctx")),
            P(("fsdp", "ctx")),
        ),
        check_vma=False,
    )
```

```python
import jax
import jax.numpy as jnp
from jax import lax
from jax.experimental import pallas as pl
from jax.experimental.pallas import tpu as pltpu
from jax.sharding import PartitionSpec as P


HD = 64
SLOT_MB = 4


epsilon = 1e-05


def tp_total(partial_sum):
    return lax.psum(partial_sum, "tp")


def layer_norm(summed, gain_row, shift_row):
    center = summed - jnp.mean(summed, axis=-1, keepdims=True)
    inverse = lax.rsqrt(jnp.mean(center * center, axis=-1, keepdims=True) + epsilon)
    normed = center * inverse
    return (normed * gain_row + shift_row, normed, inverse)


def norm_back(incoming, normed, inverse, gain_row):
    scaled = incoming * gain_row
    result = inverse * (
        scaled
        - jnp.mean(scaled, axis=-1, keepdims=True)
        - normed * jnp.mean(scaled * normed, axis=-1, keepdims=True)
    )
    return (result, jnp.sum(incoming * normed, axis=0), jnp.sum(incoming, axis=0))


def attn_scores(queries, keys_all, key_valid, score_scale):
    raw_scores = (
        jnp.einsum("bqhe,bkhe->bhqk", queries, keys_all, preferred_element_type=jnp.float32)
        * score_scale
    )
    return jnp.where(key_valid[:, None, None, :], raw_scores, -1e30)


def on_device(
    hidden_in,
    lengths,
    cotangent,
    w_qkv,
    b_qv,
    w_out,
    b_out,
    gain_one,
    shift_one,
    w_in,
    b_in,
    w_down,
    b_down,
    gain_two,
    shift_two,
):
    local_slots, row_count, model_width = hidden_in.shape
    slot_batch = SLOT_MB
    micro_count = local_slots // slot_batch
    flat_rows = slot_batch * row_count
    key_count = row_count * lax.axis_size("ctx")
    local_width = w_qkv.shape[2]
    head_count = local_width // HD
    score_scale = HD ** (-0.5)
    row_place = lax.axis_index("ctx") * row_count + jnp.arange(row_count, dtype=jnp.int32)
    key_place = jnp.arange(key_count, dtype=jnp.int32)
    bias_three = jnp.stack([b_qv[0], jnp.zeros_like(b_qv[0]), b_qv[1]]).astype(jnp.float32)
    bias_in = b_in.astype(jnp.float32)
    bias_grads = (jnp.zeros((2, local_width), jnp.float32), jnp.zeros(b_in.shape, jnp.float32))
    outputs = []
    input_grads = []
    for micro_index in range(micro_count):
        gathered = (
            lax.all_gather(w_qkv, ("fsdp", "ctx"), axis=0, tiled=True),
            lax.all_gather(w_out, ("fsdp", "ctx"), axis=1, tiled=True),
            lax.all_gather(w_in, ("fsdp", "ctx"), axis=0, tiled=True),
            lax.all_gather(w_down, ("fsdp", "ctx"), axis=1, tiled=True),
            lax.all_gather(b_out, ("fsdp", "ctx"), axis=0, tiled=True),
            lax.all_gather(gain_one, ("fsdp", "ctx"), axis=0, tiled=True),
            lax.all_gather(shift_one, ("fsdp", "ctx"), axis=0, tiled=True),
            lax.all_gather(b_down, ("fsdp", "ctx"), axis=0, tiled=True),
            lax.all_gather(gain_two, ("fsdp", "ctx"), axis=0, tiled=True),
            lax.all_gather(shift_two, ("fsdp", "ctx"), axis=0, tiled=True),
        )
        full_qkv, full_out, full_in, full_down = (
            gathered[0],
            gathered[1],
            gathered[2],
            gathered[3],
        )
        full_bout = gathered[4].astype(jnp.float32)
        full_gain_one = gathered[5].astype(jnp.float32)
        full_shift_one = gathered[6].astype(jnp.float32)
        full_bdown = gathered[7].astype(jnp.float32)
        full_gain_two = gathered[8].astype(jnp.float32)
        full_shift_two = gathered[9].astype(jnp.float32)
        first_slot = micro_index * slot_batch
        tokens = hidden_in[first_slot : first_slot + slot_batch].reshape(flat_rows, model_width)
        length = lengths[first_slot : first_slot + slot_batch]
        row_valid = (row_place[None, :] < length[:, None]).astype(jnp.float32).reshape(flat_rows)
        key_valid = key_place[None, :] < length[:, None]
        qkv_local = (
            jnp.einsum("sd,dcf->scf", tokens, full_qkv, preferred_element_type=jnp.float32)
            + bias_three
        ).astype(jnp.bfloat16)
        kv_local = qkv_local[:, 1:].reshape(slot_batch, row_count, 2, local_width)
        key_value = lax.all_gather(kv_local, "ctx", axis=1, tiled=True)
        queries = qkv_local[:, 0].reshape(slot_batch, row_count, head_count, HD)
        keys_all = key_value[:, :, 0].reshape(slot_batch, key_count, head_count, HD)
        values_all = key_value[:, :, 1].reshape(slot_batch, key_count, head_count, HD)
        scores = attn_scores(queries, keys_all, key_valid, score_scale)
        highest = jnp.max(scores, axis=-1, keepdims=True)
        exponent = jnp.exp(scores - highest)
        denominator = jnp.sum(exponent, axis=-1, keepdims=True)
        log_total = highest + jnp.log(denominator)
        probs_low = (exponent / denominator).astype(jnp.bfloat16)
        context = (
            jnp.einsum("bhqk,bkhe->bqhe", probs_low, values_all, preferred_element_type=jnp.float32)
            .astype(jnp.bfloat16)
            .reshape(flat_rows, local_width)
        )
        attended = (
            tp_total(jnp.dot(context, full_out, preferred_element_type=jnp.float32)) + full_bout
        )
        first_out, normed_one, inverse_one = layer_norm(
            tokens.astype(jnp.float32) + attended, full_gain_one, full_shift_one
        )
        first_low = first_out.astype(jnp.bfloat16)
        pre_act = jnp.dot(first_low, full_in, preferred_element_type=jnp.float32) + bias_in
        activated = jax.nn.gelu(pre_act, approximate=False).astype(jnp.bfloat16)
        branch = (
            tp_total(jnp.dot(activated, full_down, preferred_element_type=jnp.float32)) + full_bdown
        )
        result, normed_two, inverse_two = layer_norm(
            first_out + branch, full_gain_two, full_shift_two
        )
        outputs.append(result.astype(jnp.bfloat16).reshape(slot_batch, row_count, model_width))
        incoming = (
            cotangent[first_slot : first_slot + slot_batch]
            .reshape(flat_rows, model_width)
            .astype(jnp.float32)
            * row_valid[:, None]
        )
        grad_two, grad_gain_two, grad_shift_two = norm_back(
            incoming, normed_two, inverse_two, full_gain_two
        )
        grad_branch = grad_two.astype(jnp.bfloat16)
        grad_bdown = jnp.sum(grad_branch.astype(jnp.float32), axis=0)
        grad_wdown = jnp.einsum(
            "sf,sd->fd", activated, grad_branch, preferred_element_type=jnp.float32
        )
        grad_act = jnp.einsum(
            "sd,fd->sf", grad_branch, full_down, preferred_element_type=jnp.float32
        )
        _, gelu_back = jax.vjp(
            lambda inner_value: jax.nn.gelu(inner_value, approximate=False), pre_act
        )
        grad_pre = gelu_back(grad_act)[0].astype(jnp.bfloat16)
        grad_win = jnp.einsum("sd,sf->df", first_low, grad_pre, preferred_element_type=jnp.float32)
        grad_bin = jnp.sum(grad_pre.astype(jnp.float32), axis=0)
        grad_first = grad_two + tp_total(
            jnp.einsum("sf,df->sd", grad_pre, full_in, preferred_element_type=jnp.float32)
        )
        grad_one, grad_gain_one, grad_shift_one = norm_back(
            grad_first, normed_one, inverse_one, full_gain_one
        )
        grad_attended = grad_one.astype(jnp.bfloat16)
        grad_bout = jnp.sum(grad_attended.astype(jnp.float32), axis=0)
        grad_wout = jnp.einsum(
            "sf,sd->fd", context, grad_attended, preferred_element_type=jnp.float32
        )
        grad_context = (
            jnp.einsum("sd,fd->sf", grad_attended, full_out, preferred_element_type=jnp.float32)
            .astype(jnp.bfloat16)
            .reshape(slot_batch, row_count, head_count, HD)
        )
        scores_again = attn_scores(queries, keys_all, key_valid, score_scale)
        weights_back = jnp.exp(scores_again - log_total)
        grad_probs = jnp.einsum(
            "bqhe,bkhe->bhqk", grad_context, values_all, preferred_element_type=jnp.float32
        )
        grad_scores = (
            weights_back * (grad_probs - jnp.sum(grad_probs * weights_back, axis=-1, keepdims=True))
        ).astype(jnp.bfloat16)
        grad_query = (
            jnp.einsum("bhqk,bkhe->bqhe", grad_scores, keys_all, preferred_element_type=jnp.float32)
            * score_scale
        )
        grad_key = (
            jnp.einsum("bhqk,bqhe->bkhe", grad_scores, queries, preferred_element_type=jnp.float32)
            * score_scale
        )
        grad_value = jnp.einsum(
            "bhqk,bqhe->bkhe",
            weights_back.astype(jnp.bfloat16),
            grad_context,
            preferred_element_type=jnp.float32,
        )
        key_value_terms = jnp.stack(
            [
                grad_key.reshape(slot_batch, key_count, local_width),
                grad_value.reshape(slot_batch, key_count, local_width),
            ],
            axis=2,
        )
        key_value_grad = lax.psum_scatter(key_value_terms, "ctx", scatter_dimension=1, tiled=True)
        grad_qkv = (
            jnp.concatenate(
                [grad_query.reshape(slot_batch, row_count, 1, local_width), key_value_grad], axis=2
            )
            .astype(jnp.bfloat16)
            .reshape(flat_rows, 3, local_width)
        )
        grad_wqkv = jnp.einsum("sd,scf->dcf", tokens, grad_qkv, preferred_element_type=jnp.float32)
        qkv_sums = jnp.sum(grad_qkv.astype(jnp.float32), axis=0)
        grad_bqv = jnp.stack([qkv_sums[0], qkv_sums[2]])
        grad_tokens = grad_one + tp_total(
            jnp.einsum("scf,dcf->sd", grad_qkv, full_qkv, preferred_element_type=jnp.float32)
        )
        input_grads.append(
            grad_tokens.astype(jnp.bfloat16).reshape(slot_batch, row_count, model_width)
        )
        bias_grads = (bias_grads[0] + grad_bqv, bias_grads[1] + grad_bin)
        pieces = (
            lax.psum_scatter(grad_wqkv, ("fsdp", "ctx"), scatter_dimension=0, tiled=True),
            lax.psum_scatter(grad_wout, ("fsdp", "ctx"), scatter_dimension=1, tiled=True),
            lax.psum_scatter(grad_win, ("fsdp", "ctx"), scatter_dimension=0, tiled=True),
            lax.psum_scatter(grad_wdown, ("fsdp", "ctx"), scatter_dimension=1, tiled=True),
            lax.psum_scatter(grad_bout, ("fsdp", "ctx"), scatter_dimension=0, tiled=True),
            lax.psum_scatter(grad_gain_one, ("fsdp", "ctx"), scatter_dimension=0, tiled=True),
            lax.psum_scatter(grad_shift_one, ("fsdp", "ctx"), scatter_dimension=0, tiled=True),
            lax.psum_scatter(grad_bdown, ("fsdp", "ctx"), scatter_dimension=0, tiled=True),
            lax.psum_scatter(grad_gain_two, ("fsdp", "ctx"), scatter_dimension=0, tiled=True),
            lax.psum_scatter(grad_shift_two, ("fsdp", "ctx"), scatter_dimension=0, tiled=True),
        )
        grad_shards = pieces if micro_index == 0 else jax.tree.map(jnp.add, grad_shards, pieces)
    bias_total = lax.psum((bias_grads[0], bias_grads[1]), ("fsdp", "ctx"))
    return (
        jnp.concatenate(outputs, axis=0),
        jnp.concatenate(input_grads, axis=0),
        grad_shards[0],
        bias_total[0],
        grad_shards[1],
        grad_shards[4],
        grad_shards[5],
        grad_shards[6],
        grad_shards[2],
        bias_total[1],
        grad_shards[3],
        grad_shards[7],
        grad_shards[8],
        grad_shards[9],
    )


MESH = pl.DeviceIdType.MESH
ANY = pl.BlockSpec(memory_space=pl.ANY)
VM = pl.BlockSpec(memory_space=pltpu.VMEM)


class Place:
    def __init__(self):
        f, c, t = lax.axis_index("fsdp"), lax.axis_index("ctx"), lax.axis_index("tp")
        self.f, self.c, self.t = f, c, t
        core = c % 2
        self.core, self.y = core, c // 2
        self.c_core = c + 1 - 2 * core
        self.c_y = (c + 2) % 4
        self.x_dev = (1 - f, c, t)
        self.y_dev = (f, self.c_y, t)
        self.core_dev = (f, self.c_core, t)
        self.own = 4 * f + c
        self.fc_x = 4 * (1 - f) + c
        self.fc_y = 4 * f + self.c_y
        self.fc_d = 4 * (1 - f) + self.c_y

    def z_dev(self, step):
        return (self.f, self.c, (self.t + step) % 4)

    def c_dev(self, step):
        return (self.f, (self.c + step) % 4, self.t)

    def barrier(self):
        sem = pltpu.get_barrier_semaphore()
        devs = [self.z_dev(s) for s in (1, 2, 3)] + [self.x_dev] + [self.c_dev(s) for s in (1, 2, 3)]
        for dev in devs:
            pl.semaphore_signal(sem, inc=1, device_id=dev, device_id_type=MESH)
        pl.semaphore_wait(sem, len(devs))


class Sends:
    def __init__(self, sems):
        self.sems, self.list = sems, []

    def start(self, src, dst, rsem, dev, cond=None):
        copy = pltpu.make_async_remote_copy(
            src_ref=src, dst_ref=dst, send_sem=self.sems.at[len(self.list)], recv_sem=rsem,
            device_id=dev, device_id_type=MESH)
        self.list.append((copy, cond))
        if cond is None:
            copy.start()
        else:
            pl.when(cond)(copy.start)

    def finish(self):
        for copy, cond in self.list:
            if cond is None:
                copy.wait_send()
            else:
                pl.when(cond)(copy.wait_send)


def arrived(ref, rsem, dev):
    pltpu.make_async_remote_copy(
        src_ref=ref, dst_ref=ref, send_sem=rsem, recv_sem=rsem, device_id=dev, device_id_type=MESH
    ).wait_recv()


def gather_kernel(hid, *refs):
    nk = 4
    shard = refs[:nk]
    out = refs[nk:2 * nk]
    x_out = refs[2 * nk]
    ssem, rsem, xsem, lsem = refs[2 * nk + 1:]
    at = Place()
    at.barrier()
    sends = Sends(ssem)
    local = []
    for k in range(nk):
        local.append(pltpu.make_async_copy(shard[k], out[k].at[at.t, at.own], lsem.at[k]))
    local.append(pltpu.make_async_copy(hid.at[4 * at.t + at.c], x_out.at[at.c], lsem.at[nk]))
    for copy in local:
        copy.start()

    def piece(k, t, fc):
        return out[k].at[t, fc], rsem.at[k, t, fc]

    for s in (2, 3, 1):
        sends.start(hid.at[4 * at.t + (at.c + s) % 4], x_out.at[at.c], xsem.at[at.c], at.c_dev(s))
    for k in range(nk):
        for s in (1, 2, 3):
            dst, sem = piece(k, at.t, at.own)
            sends.start(shard[k], dst, sem, at.z_dev(s))
        if k == 1:
            for kk in (0, 1):
                dst, sem = piece(kk, at.t, at.own)
                for dev in (at.x_dev, at.y_dev, at.core_dev):
                    sends.start(shard[kk], dst, sem, dev)

    def forward(k, t, fc, devs):
        ref, sem = piece(k, t, fc)
        for dev in devs:
            sends.start(ref, ref, sem, dev)

    def z_in(k, s):
        tt = (at.t + s) % 4
        if s:
            arrived(*piece(k, tt, at.own), at.x_dev)
            forward(k, tt, at.own, (at.x_dev, at.y_dev, at.core_dev))
        elif k > 1:
            dst, sem = piece(k, at.t, at.own)
            for dev in (at.x_dev, at.y_dev, at.core_dev):
                sends.start(shard[k], dst, sem, dev)

    def to_x(k, s):
        return s % 2 == 1 or (k == 1 and s == 2)

    def xy_in(k, s):
        tt = (at.t + s) % 4
        arrived(*piece(k, tt, at.fc_x), at.x_dev)
        forward(k, tt, at.fc_x, (at.core_dev,) if to_x(k, s) else (at.y_dev, at.core_dev))
        arrived(*piece(k, tt, at.fc_y), at.x_dev)
        forward(k, tt, at.fc_y, (at.x_dev, at.core_dev) if to_x(k, s) else (at.core_dev,))

    def d_in(k, s):
        tt = (at.t + s) % 4
        arrived(*piece(k, tt, at.fc_d), at.x_dev)
        forward(k, tt, at.fc_d, (at.core_dev,))

    steps = [(k, s) for k in range(nk) for s in range(4)]
    n = len(steps)
    ahead = 3
    for i in range(n + ahead + 1):
        if i < n:
            z_in(*steps[i])
        if ahead <= i < n + ahead:
            xy_in(*steps[i - ahead])
        if ahead + 1 <= i:
            d_in(*steps[i - ahead - 1])
    for s in (1, 2, 3):
        c = (at.c + s) % 4
        arrived(x_out.at[c], xsem.at[c], at.x_dev)
    for k in range(nk):
        for s in range(4):
            for chip in range(4):
                arrived(*piece(k, (at.t + s) % 4, 2 * chip + 1 - at.core), at.x_dev)
    for copy in local:
        copy.wait()
    sends.finish()


def gather_all(hid, shards):
    n_send = 4 * 31 + 3
    out_shape = [jax.ShapeDtypeStruct((4, 8) + s.shape, s.dtype) for s in shards]
    out_shape += [jax.ShapeDtypeStruct((4,) + hid.shape[1:], hid.dtype)]
    return pl.pallas_call(
        gather_kernel,
        out_shape=out_shape,
        in_specs=[ANY] + [VM] * 4,
        out_specs=[ANY] * 5,
        scratch_shapes=[
            pltpu.SemaphoreType.DMA((n_send,)),
            pltpu.SemaphoreType.DMA((4, 4, 8)),
            pltpu.SemaphoreType.DMA((4,)),
            pltpu.SemaphoreType.DMA((5,)),
        ],
        compiler_params=pltpu.CompilerParams(collective_id=0, has_side_effects=True),
        name="gather_all",
    )(hid, *shards)


def reduce_kernel(*refs):
    nk = 3
    grads = refs[:nk]
    vec, o_slots = refs[nk], refs[nk + 1:nk + 2]
    total = refs[nk + 2:2 * nk + 2]
    vec_out, outs = refs[2 * nk + 2], refs[2 * nk + 3:2 * nk + 4]
    rc, own, bx, by, dx, dy, bz, vbuf, ssem, csem, bsem, zsem, vsem, osem, lsem = refs[2 * nk + 4:]
    at = Place()
    at.barrier()
    sends = Sends(ssem)
    chips = (at.fc_d, at.fc_x, at.fc_y, at.own)
    local = []

    for i in range(1):
        copy = pltpu.make_async_copy(o_slots[i].at[at.c], outs[i].at[4 * at.t + at.c], lsem.at[i])
        copy.start()
        local.append(copy)

    def slot_out(i):
        slot = 4 * at.t + at.c
        for s in (2, 1, 3):
            sends.start(o_slots[i].at[(at.c + s) % 4], outs[i].at[slot], osem.at[i, slot], at.c_dev(s))

    def along(i, hop, src_c, src=None):
        slot_r = 4 * ((at.t - hop) % 4) + src_c
        slot_l = 4 * ((at.t + hop) % 4) + src_c
        if hop:
            @pl.when(at.t >= hop)
            def _():
                arrived(outs[i].at[slot_r], osem.at[i, slot_r], at.x_dev)

            @pl.when(at.t + hop <= 3)
            def _():
                arrived(outs[i].at[slot_l], osem.at[i, slot_l], at.x_dev)
        if hop < 3:
            ref = outs[i].at[slot_r] if src is None else src
            sends.start(ref, outs[i].at[slot_r], osem.at[i, slot_r], at.z_dev(1), (at.t >= hop) & (at.t < 3))
            ref = outs[i].at[slot_l] if src is None else src
            sends.start(ref, outs[i].at[slot_l], osem.at[i, slot_l], at.z_dev(3), (at.t + hop <= 3) & (at.t > 0))

    def along_own(i, s):
        c = (at.c + s) % 4
        if s == 0:
            along(i, 0, at.c, o_slots[i].at[at.c])
        else:
            slot = 4 * at.t + c
            arrived(outs[i].at[slot], osem.at[i, slot], at.x_dev)
            along(i, 0, c)

    def core_out(k):
        for r, fc in enumerate(chips):
            other = fc + 1 - 2 * at.core
            sends.start(grads[k].at[:, other], rc.at[k, r], csem.at[k, r], at.core_dev)

    def add_core(k, r):
        arrived(rc.at[k, r], csem.at[k, r], at.x_dev)
        fc = chips[r]

        @pl.loop(0, 4)
        def _(t):
            both = grads[k][t, fc].astype(jnp.float32) + rc[k, r, t].astype(jnp.float32)
            rc[k, r, t] = both.astype(jnp.bfloat16)

    def diag_out(k):
        add_core(k, 0)
        sends.start(rc.at[k, 0, pl.ds(0, 2)], dx.at[k], bsem.at[k, 0], at.x_dev)
        sends.start(rc.at[k, 0, pl.ds(2, 2)], dy.at[k], bsem.at[k, 1], at.y_dev)

    def side_out(k):
        add_core(k, 1)
        sends.start(rc.at[k, 1, pl.ds(0, 2)], bx.at[k, pl.ds(0, 2)], bsem.at[k, 2], at.x_dev)
        add_core(k, 2)
        sends.start(rc.at[k, 2, pl.ds(2, 2)], by.at[k, pl.ds(2, 2)], bsem.at[k, 3], at.y_dev)

    def relay(k):
        arrived(dy.at[k], bsem.at[k, 1], at.x_dev)

        @pl.loop(0, 2)
        def _(t):
            both = rc[k, 1, t + 2].astype(jnp.float32) + dy[k, t].astype(jnp.float32)
            rc[k, 1, t + 2] = both.astype(jnp.bfloat16)

        sends.start(rc.at[k, 1, pl.ds(2, 2)], bx.at[k, pl.ds(2, 2)], bsem.at[k, 4], at.x_dev)
        arrived(dx.at[k], bsem.at[k, 0], at.x_dev)

        @pl.loop(0, 2)
        def _(t):
            both = rc[k, 2, t].astype(jnp.float32) + dx[k, t].astype(jnp.float32)
            rc[k, 2, t] = both.astype(jnp.bfloat16)

        sends.start(rc.at[k, 2, pl.ds(0, 2)], by.at[k, pl.ds(0, 2)], bsem.at[k, 5], at.y_dev)

    def own_sum(k):
        add_core(k, 3)
        arrived(bx.at[k, pl.ds(0, 2)], bsem.at[k, 2], at.x_dev)
        arrived(by.at[k, pl.ds(2, 2)], bsem.at[k, 3], at.x_dev)
        arrived(bx.at[k, pl.ds(2, 2)], bsem.at[k, 4], at.x_dev)
        arrived(by.at[k, pl.ds(0, 2)], bsem.at[k, 5], at.x_dev)

        @pl.loop(0, 4)
        def _(t):
            four = rc[k, 3, t].astype(jnp.float32) + bx[k, t].astype(jnp.float32) + by[k, t].astype(jnp.float32)
            own[k, t] = four.astype(jnp.bfloat16)

        for s in (2, 1, 3):
            sends.start(own.at[k, (at.t + s) % 4], bz.at[k, s - 1], zsem.at[k, s - 1], at.z_dev(s))

    def last(k):
        for s in (1, 2, 3):
            arrived(bz.at[k, s - 1], zsem.at[k, s - 1], at.x_dev)

        @pl.loop(0, 6)
        def _(i):
            rows = pl.ds(pl.multiple_of(i * 16, 16), 16)
            value = own[k, at.t, rows].astype(jnp.float32)
            for s in range(3):
                value = value + bz[k, s, rows].astype(jnp.float32)
            total[k][rows] = value

    def vec_step(i):
        if i:
            arrived(vbuf.at[i - 1], vsem.at[i - 1], at.x_dev)
            vbuf[2 + i] = (vec[...] if i == 1 else vbuf[1 + i]) + vbuf[i - 1]
        if i < 3:
            sends.start(vec if i == 0 else vbuf.at[2 + i], vbuf.at[i], vsem.at[i], (at.core_dev, at.x_dev, at.y_dev)[i])
        else:
            for s in (1, 2, 3):
                sends.start(vbuf.at[5], vbuf.at[6 + at.t], vsem.at[3 + at.t], at.z_dev(s))

    def vec_last():
        for s in (1, 2, 3):
            t = (at.t + s) % 4
            arrived(vbuf.at[6 + t], vsem.at[3 + t], at.x_dev)
        vbuf[6 + at.t] = vbuf[5]
        vec_out[...] = vbuf[6] + vbuf[7] + vbuf[8] + vbuf[9]

    slot_out(0)
    core_out(2)
    along_own(0, 0)
    core_out(1)
    core_out(0)
    vec_step(0)
    diag_out(2)
    side_out(2)
    for s in (1, 3, 2):
        along_own(0, s)
    jobs = [lambda: diag_out(1), lambda: side_out(1), lambda: relay(2), lambda: diag_out(0), lambda: vec_step(1),
            lambda: side_out(0), lambda: relay(1), lambda: vec_step(2), lambda: own_sum(2), lambda: relay(0),
            lambda: vec_step(3), lambda: own_sum(1), lambda: last(2), lambda: own_sum(0), lambda: last(1),
            lambda: vec_last(), lambda: last(0)]
    hops = [(0, hop, s) for hop in (1, 2, 3) for s in range(4)]
    n = max(len(jobs), len(hops))
    for j in range(n):
        if j < len(jobs):
            jobs[j]()
        if j < len(hops):
            i, hop, s = hops[j]
            along(i, hop, (at.c + (0, 1, 3, 2)[s]) % 4)
    for copy in local:
        copy.wait()
    sends.finish()


def reduce_all(grads, vec, o_slots, slot_count):
    rows, width = grads[0].shape[2:]
    bf = jnp.bfloat16
    dma = pltpu.SemaphoreType.DMA
    n_send = 3 * (4 + 2 + 2 + 2 + 3) + 6 + 3 + 24
    out_shape = [jax.ShapeDtypeStruct((rows, width), jnp.float32)] * 3
    out_shape += [jax.ShapeDtypeStruct(vec.shape, jnp.float32)]
    out_shape += [jax.ShapeDtypeStruct((slot_count,) + o_slots[0].shape[1:], bf)]
    return pl.pallas_call(
        reduce_kernel,
        out_shape=out_shape,
        in_specs=[VM] * 5,
        out_specs=[VM] * 4 + [ANY],
        scratch_shapes=[
            pltpu.VMEM((3, 4, 4, rows, width), bf),
            pltpu.VMEM((3, 4, rows, width), bf),
            pltpu.VMEM((3, 4, rows, width), bf),
            pltpu.VMEM((3, 4, rows, width), bf),
            pltpu.VMEM((3, 2, rows, width), bf),
            pltpu.VMEM((3, 2, rows, width), bf),
            pltpu.VMEM((3, 3, rows, width), bf),
            pltpu.VMEM((10,) + vec.shape, jnp.float32),
            dma((n_send,)), dma((3, 4)), dma((3, 6)), dma((3, 3)), dma((7,)), dma((1, slot_count)), dma((1,)),
        ],
        compiler_params=pltpu.CompilerParams(collective_id=1, has_side_effects=True,
                                             vmem_limit_bytes=60 * 1024 * 1024),
        name="reduce_all",
    )(*grads, vec, *o_slots)


def one_slot(tokens, length, cotangent, mix, w_in, w_down_t, small):
    f32, bf16 = jnp.float32, jnp.bfloat16
    rows, _ = tokens.shape
    groups, _, width = mix.shape
    part = width // 4
    per = part // HD
    score_scale = HD ** (-0.5)
    spot = jnp.arange(rows, dtype=jnp.int32)
    valid = spot < length
    small = small.astype(f32)
    bias_in, bias_qv = small[:, 0, 0], small[:, 0, 1]
    bout, gain_one, shift_one, bdown, gain_two, shift_two = [jnp.sum(small[0, :, 2 + i], axis=0) for i in range(6)]
    w_qkv = mix[:, :, : 3 * part]
    w_out_t = mix[:, :, 3 * part :]
    qkv = jnp.einsum("sd,tdn->tsn", tokens, w_qkv, preferred_element_type=f32) + bias_qv[:, None, : 3 * part]
    qkv = qkv.astype(bf16).reshape(groups, rows, 3, per, HD)
    queries, keys, values = qkv[:, :, 0], qkv[:, :, 1], qkv[:, :, 2]
    scores = jnp.einsum("tqhe,tkhe->thqk", queries, keys, preferred_element_type=f32) * score_scale
    scores = jnp.where(valid[None, None, None, :], scores, -1e30)
    highest = jnp.max(scores, axis=-1, keepdims=True)
    exponent = jnp.exp(scores - highest)
    denominator = jnp.sum(exponent, axis=-1, keepdims=True)
    probs = exponent / denominator
    probs_low = probs.astype(bf16)
    context = jnp.einsum("thqk,tkhe->tqhe", probs_low, values, preferred_element_type=f32).astype(bf16)
    context = context.reshape(groups, rows, part)
    attended = jnp.einsum("tsf,tdf->sd", context, w_out_t, preferred_element_type=f32) + bout
    first_out, normed_one, inverse_one = layer_norm(tokens.astype(f32) + attended, gain_one, shift_one)
    first_low = first_out.astype(bf16)
    pre_act = jnp.einsum("sd,tdf->tsf", first_low, w_in, preferred_element_type=f32) + bias_in[:, None, :]
    half = 0.5 * (1.0 + lax.erf(pre_act * (2.0 ** -0.5)))
    activated = (pre_act * half).astype(bf16)
    slope = half + pre_act * jnp.exp(-0.5 * pre_act * pre_act) * 0.3989422804014327
    branch = jnp.einsum("tsf,tdf->sd", activated, w_down_t, preferred_element_type=f32) + bdown
    result, normed_two, inverse_two = layer_norm(first_out + branch, gain_two, shift_two)
    incoming = cotangent.astype(f32) * valid.astype(f32)[:, None]
    grad_two, g_gain_two, g_shift_two = norm_back(incoming, normed_two, inverse_two, gain_two)
    grad_branch = grad_two.astype(bf16)
    g_bdown = jnp.sum(grad_branch.astype(f32), axis=0)
    g_down_t = jnp.einsum("sd,tsf->tdf", grad_branch, activated, preferred_element_type=f32).astype(bf16)
    grad_act = jnp.einsum("sd,tdf->tsf", grad_branch, w_down_t, preferred_element_type=f32)
    grad_pre = (grad_act * slope).astype(bf16)
    g_in = jnp.einsum("sd,tsf->tdf", first_low, grad_pre, preferred_element_type=f32).astype(bf16)
    g_bin = jnp.sum(grad_pre.astype(f32), axis=1)
    grad_first = jnp.einsum("tsf,tdf->sd", grad_pre, w_in, preferred_element_type=f32)
    grad_first = grad_two + grad_first
    grad_one, g_gain_one, g_shift_one = norm_back(grad_first, normed_one, inverse_one, gain_one)
    grad_attended = grad_one.astype(bf16)
    g_bout = jnp.sum(grad_attended.astype(f32), axis=0)
    g_out_t = jnp.einsum("sd,tsf->tdf", grad_attended, context, preferred_element_type=f32).astype(bf16)
    grad_context = jnp.einsum("sd,tdf->tsf", grad_attended, w_out_t, preferred_element_type=f32).astype(bf16)
    grad_context = grad_context.reshape(groups, rows, per, HD)
    grad_probs = jnp.einsum("tqhe,tkhe->thqk", grad_context, values, preferred_element_type=f32)
    grad_scores = (probs * (grad_probs - jnp.sum(grad_probs * probs, axis=-1, keepdims=True))).astype(bf16)
    grad_query = jnp.einsum("thqk,tkhe->tqhe", grad_scores, keys, preferred_element_type=f32) * score_scale
    grad_key = jnp.einsum("thqk,tqhe->tkhe", grad_scores, queries, preferred_element_type=f32) * score_scale
    grad_value = jnp.einsum("thqk,tqhe->tkhe", probs_low, grad_context, preferred_element_type=f32)
    grad_qkv = jnp.concatenate(
        [part_grad.astype(bf16).reshape(groups, rows, part) for part_grad in (grad_query, grad_key, grad_value)],
        axis=2,
    )
    g_qkv = jnp.einsum("sd,tsn->tdn", tokens, grad_qkv, preferred_element_type=f32).astype(bf16)
    g_bqv = jnp.sum(grad_qkv.astype(f32), axis=1)
    grad_tokens = jnp.einsum("tsn,tdn->sd", grad_qkv, w_qkv, preferred_element_type=f32)
    grad_tokens = grad_one + grad_tokens
    g_mix = jnp.concatenate([g_qkv, g_out_t], axis=2)
    vec = jnp.concatenate(
        [
            g_bin,
            jnp.pad(g_bqv, ((0, 0), (0, part))),
            jnp.stack([g_bout, g_gain_one, g_shift_one, g_bdown, g_gain_two, g_shift_two]),
            jnp.zeros((2, width), f32),
        ]
    )
    return result.astype(bf16), grad_tokens.astype(bf16), g_mix, g_in, g_down_t, vec


def ring(axis, step):
    size = lax.axis_size(axis)
    return [(i, (i + step) % size) for i in range(size)]


def slot_in(blocks):
    ctx = lax.axis_size("ctx")
    c, t = lax.axis_index("ctx"), lax.axis_index("tp")
    take = lambda member: lax.dynamic_index_in_dim(blocks, ctx * t + member % ctx, keepdims=False)
    whole = jnp.zeros((ctx,) + blocks.shape[1:], blocks.dtype)
    for step in range(ctx):
        part = take(c + step)
        if step:
            part = lax.ppermute(part, "ctx", ring("ctx", step))
        whole = lax.dynamic_update_index_in_dim(whole, part, (c - step) % ctx, 0)
    return whole.reshape(-1, blocks.shape[2])


def slot_back(whole, slot_count):
    ctx, tp = lax.axis_size("ctx"), lax.axis_size("tp")
    c, t = lax.axis_index("ctx"), lax.axis_index("tp")
    four = jnp.zeros_like(whole)
    for step in range(ctx):
        part = lax.dynamic_index_in_dim(whole, (c + step) % ctx, keepdims=False)
        if step:
            part = lax.ppermute(part, "ctx", ring("ctx", step))
        four = lax.dynamic_update_index_in_dim(four, part, (c - step) % ctx, 0)
    out = jnp.zeros((tp,) + four.shape, four.dtype)
    for step in range(tp):
        part = four
        if step:
            part = lax.ppermute(four, "tp", ring("tp", step))
        out = lax.dynamic_update_index_in_dim(out, part, (t - step) % tp, 0)
    return out.reshape((slot_count,) + whole.shape[1:])


def slot_per_device(
    hidden_in, lengths, cotangent, w_qkv, b_qv, w_out, b_out, gain_one, shift_one, w_in, b_in, w_down, b_down,
    gain_two, shift_two,
):
    slot_count, block, model_width = hidden_in.shape
    rows, _, part = w_qkv.shape
    f, c, t = lax.axis_index("fsdp"), lax.axis_index("ctx"), lax.axis_index("tp")
    ctx = lax.axis_size("ctx")
    own = f * ctx + c
    mix = jnp.concatenate([w_qkv.reshape(rows, 3 * part), w_out.T], axis=1)
    vectors = jnp.stack([b_out, gain_one, shift_one, b_down, gain_two, shift_two])
    placed = jnp.where(
        jnp.arange(model_width, dtype=jnp.int32)[None, :] // rows == own, jnp.tile(vectors, (1, model_width // rows)), 0
    ).astype(jnp.bfloat16)
    gap = jnp.zeros((part,), jnp.bfloat16)
    small = jnp.concatenate(
        [
            b_in[None],
            jnp.concatenate([b_qv[0], gap, b_qv[1], gap])[None],
            placed,
            jnp.zeros((8, model_width), jnp.bfloat16),
        ]
    )
    cot = slot_in(cotangent)
    small_all, mix_all, in_all, down_all, tokens = gather_all(
        hidden_in, (small, mix, w_in, w_down.T)
    )
    full = lambda g: g.reshape(g.shape[0], model_width, g.shape[3])
    length = lax.dynamic_index_in_dim(lengths, t * ctx + c, keepdims=False)
    result, grad_tokens, g_mix, g_in, g_down, vec = one_slot(
        tokens.reshape(ctx * block, model_width), length, cot,
        full(mix_all), full(in_all), full(down_all), small_all,
    )
    split = lambda g: g.reshape(g.shape[0], model_width // rows, rows, g.shape[2])
    back = lambda o: o.reshape(ctx, block, model_width)
    out = slot_back(back(result), slot_count)
    t_mix, t_in, t_down, t_vec, grad_in = reduce_all(
        (split(g_mix), split(g_in), split(g_down)), vec, (back(grad_tokens),), slot_count
    )
    piece = lax.dynamic_slice_in_dim(t_vec[8:14], own * rows, rows, axis=1)
    bqv = lax.dynamic_index_in_dim(t_vec, 4 + t, keepdims=False)
    bin_grad = lax.dynamic_index_in_dim(t_vec, t, keepdims=False)
    return (
        out,
        grad_in,
        t_mix[:, : 3 * part].reshape(rows, 3, part),
        jnp.stack([bqv[:part], bqv[2 * part : 3 * part]]),
        t_mix[:, 3 * part :].T,
        piece[0],
        piece[1],
        piece[2],
        t_in,
        bin_grad,
        t_down.T,
        piece[3],
        piece[4],
        piece[5],
    )


def solution(mesh):
    shape = mesh.shape
    whole_slots = (shape["fsdp"], shape["ctx"], shape["tp"]) == (2, 4, 4)
    return jax.shard_map(
        slot_per_device if whole_slots else on_device,
        mesh=mesh,
        in_specs=(
            P("fsdp", "ctx", None),
            P("fsdp"),
            P("fsdp", "ctx", None),
            P(("fsdp", "ctx"), None, "tp"),
            P(None, "tp"),
            P("tp", ("fsdp", "ctx")),
            P(("fsdp", "ctx")),
            P(("fsdp", "ctx")),
            P(("fsdp", "ctx")),
            P(("fsdp", "ctx"), "tp"),
            P("tp"),
            P("tp", ("fsdp", "ctx")),
            P(("fsdp", "ctx")),
            P(("fsdp", "ctx")),
            P(("fsdp", "ctx")),
        ),
        out_specs=(
            P("fsdp", "ctx", None),
            P("fsdp", "ctx", None),
            P(("fsdp", "ctx"), None, "tp"),
            P(None, "tp"),
            P("tp", ("fsdp", "ctx")),
            P(("fsdp", "ctx")),
            P(("fsdp", "ctx")),
            P(("fsdp", "ctx")),
            P(("fsdp", "ctx"), "tp"),
            P("tp"),
            P("tp", ("fsdp", "ctx")),
            P(("fsdp", "ctx")),
            P(("fsdp", "ctx")),
            P(("fsdp", "ctx")),
        ),
        check_vma=False,
    )
```
